32 devices in a mesh: grp: 4 (over y, x), cp: 8 (over z, core).
Axes of the slice: x: 2, y: 2, z: 4, core: 2. Of those that a mesh axis runs over, the one named last changes fastest.
Arguments:
- queries: bfloat16 [16384, 2048], P(('grp', 'cp')), parts along dimension 0, may hold values from -6 to 6
- keys: bfloat16 [16384, 1024], P(('grp', 'cp')), parts along dimension 0, may hold values from -8 to 8
- values: bfloat16 [16384, 1024], P(('grp', 'cp')), parts along dimension 0, may hold values from -6 to 6
- doc_lengths: int32 [128], P('grp'), parts along dimension 0, may hold values from 1 to 1024, 4096 in all
Outputs:
- attended: bfloat16 [16384, 2048], P(('grp', 'cp')), parts along dimension 0
The draws below stay inside these ranges and needn't reach their ends.
There are 4 independent parts, one for each index of `grp`. The reference program is written for one: setup_inputs(seed, part) draws one part's arguments, and reference() takes and returns one part's arrays. A program takes and returns all parts, laid end to end along the dimension named above; each array names one. Nothing has to cross between parts.
Inputs may be any that keep to these rules, and one draw needn't show every extreme that they name: doc_lengths sums to 4096, and its largest entry is exactly 1024.
All inputs are finite; a program needn't handle non-finite values.
Results may differ from the reference program's by a relative error of at most 0.0031.
Values may be sent and summed in bfloat16 or wider, within the bound.
A program may use at most 64 MiB of HBM per device.

```python
import math
import jax
import jax.numpy as jnp
import numpy as np
from jax import lax

HQ = 16
HK = 8
DH = 128
TOK_DEV = 512
REACH = 2
TOKENS = 4096
MAXDOC = 1024
DOCS = 32


def draw_queries(key, part):
    drawn = jnp.clip(jax.random.normal(jax.random.fold_in(key, 11), (TOKENS, HQ * DH), jnp.float32), -6.0, 6.0)
    return drawn.astype(jnp.bfloat16)


def draw_keys(key, part):
    drawn = jnp.clip(jax.random.normal(jax.random.fold_in(key, 22), (TOKENS, HK * DH), jnp.float32), -6.0, 6.0)
    return drawn.astype(jnp.bfloat16)


def shard_levels(rng, extent, shards, low, largest):
    factor_of, own = 1.0, jax.random.fold_in(rng, 6)
    for dim, blocks in shards:
        draws = jnp.exp(jax.random.uniform(jax.random.fold_in(own, dim), (blocks,), jnp.float32, low / len(shards), largest / len(shards)))
        factor_of = factor_of * jnp.repeat(draws, extent[dim] // blocks).reshape([-1 if axis == dim else 1 for axis in range(len(extent))])
    return factor_of


def profile(count, total, bound, skew):
    weights = [(1 << 20) // math.isqrt(standing ** skew) + 1 for standing in range(2, count + 1)]
    surplus, given = total - bound - (count - 1), [1] * (count - 1)
    while surplus > 0:
        movable = [i for i in range(count - 1) if given[i] < bound]
        mass, remaining = sum([weights[i] for i in movable]), surplus
        for i in movable:
            extra = min(bound - given[i], max(1, remaining * weights[i] // mass), surplus)
            given[i] = given[i] + extra
            surplus = surplus - extra
    return np.array([bound] + given)


def ragged_sizes(key, number_of, total, most, skew):
    if number_of == 2:
        one = jax.random.randint(key, (), max(1, total - most), min(most, total - 1) + 1)
        return jnp.stack([one, total - one])
    lengths = jnp.asarray(profile(number_of, total, most, skew), jnp.int32)
    couples = (number_of - 1) // 2
    source_of, taker = lengths[1:1 + 2 * couples:2], lengths[2:2 + 2 * couples:2]
    room = jnp.minimum(source_of - 1, most - taker)
    passed = jax.random.randint(jax.random.fold_in(key, 1), (couples,), 0, 1 << 20) % (room + 1)
    lengths = lengths.at[1:1 + 2 * couples:2].set(source_of - passed).at[2:2 + 2 * couples:2].set(taker + passed)
    return lengths[jax.random.permutation(jax.random.fold_in(key, 2), number_of)]


def noise(rng, dims, spread, limit, shards=(), held_as=jnp.bfloat16):
    loudness = shard_levels(rng, dims, shards, -0.22, 0.18) if shards else 1.0
    array = jax.random.normal(rng, dims, jnp.float32) * spread * loudness
    return jnp.minimum(jnp.maximum(array, -limit), limit).astype(held_as)


def setup_inputs(seed: int = 0, part: int = 0) -> dict:
    arg_keys = jax.random.split(jax.random.key(seed), 5)
    part_splits = jax.random.split(jax.random.fold_in(arg_keys[4], part), 5)
    queries = draw_queries(jax.random.fold_in(jax.random.fold_in(arg_keys[4], part), 71), part)
    keys = draw_keys(jax.random.fold_in(jax.random.fold_in(arg_keys[4], part), 71), part)
    values = noise(part_splits[2], (TOKENS, HK * DH), 1.0, 6.0, ((0, 8),))
    doc_lengths = ragged_sizes(part_splits[3], DOCS, TOKENS, MAXDOC, 2).astype(jnp.int32)
    return {"queries": queries, "keys": keys, "values": values, "doc_lengths": doc_lengths}


query_scale = 144.0 ** -0.5


def doc_index(positions, doc_ends):
    return jnp.sum((positions[:, None] >= doc_ends[None, :]).astype(jnp.int32), axis=1).astype(jnp.int32)


def attend(query_rows, key_rows, value_rows, visible):
    tok_rows = query_rows.shape[0]
    key_count = key_rows.shape[0]
    groups = HQ // HK
    query_heads = query_rows.astype(jnp.float32).reshape(tok_rows, HK, groups, DH)
    key_heads = key_rows.astype(jnp.float32).reshape(key_count, HK, DH)
    value_heads = value_rows.astype(jnp.float32).reshape(key_count, HK, DH)
    scores = jnp.einsum("tkgd,wkd->kgtw", query_heads, key_heads) * query_scale
    scores = jnp.where(visible[None, None], scores, -jnp.inf)
    highest = jnp.max(scores, axis=-1, keepdims=True)
    weights = jnp.exp(scores - highest)
    totals = jnp.sum(weights, axis=-1)
    rounded = lax.optimization_barrier(weights.astype(jnp.bfloat16))
    mixed = jnp.einsum("kgtw,wkd->tkgd", rounded.astype(jnp.float32), value_heads)
    mixed = mixed / jnp.transpose(totals, (2, 0, 1))[..., None]
    return mixed.reshape(tok_rows, HQ * DH).astype(jnp.bfloat16)


def reference(queries, keys, values, doc_lengths):
    doc_ends = jnp.cumsum(doc_lengths).astype(jnp.int32)
    margin = REACH * TOK_DEV
    window = (REACH + 1) * TOK_DEV
    pad_keys = jnp.concatenate([jnp.zeros((margin, HK * DH), keys.dtype), keys], axis=0)
    pad_values = jnp.concatenate([jnp.zeros((margin, HK * DH), values.dtype), values], axis=0)

    def one_block(index):
        begin_row = (index * TOK_DEV).astype(jnp.int32)
        query_pos = begin_row + jnp.arange(TOK_DEV, dtype=jnp.int32)
        key_pos = begin_row - margin + jnp.arange(window, dtype=jnp.int32)
        same_doc = doc_index(query_pos, doc_ends)[:, None] == doc_index(key_pos, doc_ends)[None, :]
        visible = same_doc & (key_pos[None, :] <= query_pos[:, None]) & (key_pos[None, :] >= 0)
        query_rows = lax.dynamic_slice_in_dim(queries, begin_row, TOK_DEV, 0)
        key_rows = lax.dynamic_slice_in_dim(pad_keys, begin_row, window, 0)
        value_rows = lax.dynamic_slice_in_dim(pad_values, begin_row, window, 0)
        return attend(query_rows, key_rows, value_rows, visible)

    blocks = lax.map(one_block, jnp.arange(TOKENS // TOK_DEV, dtype=jnp.int32))
    return blocks.reshape(TOKENS, HQ * DH)
```

```python
import functools
import math

import jax
import jax.numpy as jnp
from jax import lax
from jax.experimental import pallas as pl
from jax.experimental.pallas import tpu as pltpu
from jax.sharding import PartitionSpec as P

HQ = 16
HK = 8
DH = 128
GROUPS = HQ // HK
WIDTH = GROUPS * DH
TILE = 128
STACK = GROUPS * TILE
MASKED = -1e30
SPLIT = HK // 2
MESH = pl.DeviceIdType.MESH

LOG2E = math.log2(math.e)
exponent_scale = 144.0 ** (-0.5) * LOG2E


def kernel(
    shards,
    lengths_ref,
    queries_ref,
    keys_ref,
    values_ref,
    out_ref,
    held,
    query_held,
    out_held,
    query_back,
    slot,
    stat_out,
    stat_in,
    bias,
    back_bias,
    lengths,
    mode,
    ones,
    part_mixed,
    part_total,
    part_high,
    lengths_sem,
    load_sem,
    query_sem,
    out_sem,
    core_send,
    core_recv,
    query_send,
    query_recv,
    slot_send,
    slot_recv,
    relay_send,
    relay_recv,
    stat_send,
    stat_recv,
):
    me = lax.axis_index("cp")
    core = lax.rem(me, 2)
    even = core == 0
    odd = core == 1
    partner = me + 1 - 2 * core
    rows = keys_ref.shape[0]
    docs = lengths_ref.shape[1]
    tiles = rows // TILE
    received = pl.ds(0, rows)
    own = pl.ds(pl.multiple_of((1 + core) * rows, rows), rows)
    has_prev = me >= 2
    has_next = me < shards - 2
    chip_begin = (me - core) * rows
    next_begin = chip_begin + 2 * rows

    def loads(head):
        lanes = pl.ds(pl.multiple_of(head * DH, DH), DH)
        return (
            pltpu.make_async_copy(keys_ref.at[:, lanes], held.at[head, 0, own], load_sem.at[head, 0]),
            pltpu.make_async_copy(values_ref.at[:, lanes], held.at[head, 1, own], load_sem.at[head, 1]),
        )

    def query_load(head):
        lanes = pl.ds(pl.multiple_of(head * WIDTH, WIDTH), WIDTH)
        return pltpu.make_async_copy(queries_ref.at[:, lanes], query_held.at[head], query_sem.at[head])

    def out_store(head):
        lanes = pl.ds(pl.multiple_of(head * WIDTH, WIDTH), WIDTH)
        return pltpu.make_async_copy(out_held.at[head], out_ref.at[:, lanes], out_sem.at[head])

    def remote(source, target, send, recv, device):
        return pltpu.make_async_remote_copy(
            src_ref=source,
            dst_ref=target,
            send_sem=send,
            recv_sem=recv,
            device_id={"cp": device},
            device_id_type=MESH,
        )

    def to_core(head):
        return remote(held.at[head, :, own], held.at[head, :, own], core_send.at[head], core_recv.at[head], partner)

    def from_core(head):
        other = pl.ds(pl.multiple_of((2 - core) * rows, rows), rows)
        return remote(held.at[head, :, other], held.at[head, :, other], core_send.at[head], core_recv.at[head], partner)

    def query_to_prev(step, side, tile):
        span = pl.ds(tile * TILE, TILE)
        return remote(
            query_held.at[side * SPLIT + step, span],
            query_back.at[step, span],
            query_send.at[side * SPLIT + step],
            query_recv.at[step, tile],
            me - 2 + side,
        )

    def query_sent(head):
        return remote(
            query_held.at[head], query_held.at[head], query_send.at[head], query_send.at[head], me - 2
        )

    def slot_to_next(step, span):
        return remote(
            slot.at[step, :, span],
            held.at[core * SPLIT + step, :, span],
            slot_send.at[step],
            slot_recv.at[step],
            me + 2,
        )

    def relay(step, side):
        head = side * SPLIT + step
        return remote(
            held.at[head, :, received], held.at[head, :, received], relay_send.at[step], relay_recv.at[step], partner
        )

    def stat_to_next(step, head):
        return remote(
            stat_out.at[step], stat_in.at[head], stat_send.at[step], stat_recv.at[head], me + 2 - core
        )

    barrier = pltpu.get_barrier_semaphore()

    def greet(device):
        pl.semaphore_signal(barrier, inc=1, device_id={"cp": device}, device_id_type=MESH)

    greet(partner)

    @pl.when(has_prev)
    def _():
        greet(me - 2)

        @pl.when(even)
        def _():
            greet(me - 1)

    @pl.when(has_next)
    def _():
        greet(me + 2)

        @pl.when(odd)
        def _():
            greet(me + 1)

    @pl.loop(0, SPLIT)
    def _(step):
        query_load(step).start()
        query_load(SPLIT + step).start()

    lengths_load = pltpu.make_async_copy(lengths_ref, lengths, lengths_sem)
    lengths_load.start()

    @pl.loop(0, HK)
    def _(head):
        for copy in loads(head):
            copy.start()

    back_peers = jnp.where(has_prev, 2 - core, 0)
    next_peers = jnp.where(has_next, 1 + core, 0)
    pl.semaphore_wait(barrier, 1 + back_peers + next_peers)

    @pl.loop(0, SPLIT)
    def _(step):
        query_load(step).wait()
        query_load(SPLIT + step).wait()

        @pl.when(jnp.logical_and(even, has_prev))
        def _():
            for tile in range(tiles):
                for side in range(2):
                    query_to_prev(step, side, tile).start()

    @pl.loop(0, HK)
    def _(head):
        for copy in loads(head):
            copy.wait()

        @pl.when(jnp.logical_or(even, head < SPLIT))
        def _():
            to_core(head).start()

    @pl.when(jnp.logical_not(has_prev))
    def _():
        held[:, :, received, :] = jnp.zeros((HK, 2, rows, DH), held.dtype)

        @pl.when(even)
        def _():
            stat_in[...] = jnp.full(stat_in.shape, MASKED, jnp.float32)

    ones[...] = jnp.ones(ones.shape, ones.dtype)

    lengths_load.wait()
    doc_row = lax.broadcasted_iota(jnp.int32, (docs, docs), 0)
    doc_lane = lax.broadcasted_iota(jnp.int32, (docs, docs), 1)
    length_row = lengths[...].astype(jnp.float32)
    length_column = jnp.sum(jnp.where(doc_row == doc_lane, length_row, 0.0), axis=1, keepdims=True)
    doc_ends = jnp.sum(jnp.where(doc_row <= doc_lane, length_column, 0.0), axis=0, keepdims=True)

    def doc_begins(positions):
        return jnp.max(jnp.where(positions >= doc_ends, doc_ends, 0.0), axis=1, keepdims=True)

    def boundary_begin(boundary):
        return doc_begins(jnp.full((8, 1), boundary, jnp.int32).astype(jnp.float32))

    def as_float(number):
        return jnp.full((1, 1), number, jnp.int32).astype(jnp.float32)

    row_iota = lax.broadcasted_iota(jnp.int32, (TILE, 1), 0)
    for tile in range(tiles):
        begins = doc_begins((next_begin + tile * TILE + row_iota).astype(jnp.float32))
        key_pos = (chip_begin + lax.broadcasted_iota(jnp.int32, (TILE, 2 * rows), 1)).astype(jnp.float32)
        back_bias[pl.ds(tile * TILE, TILE), :] = jnp.where(key_pos >= begins, 0.0, MASKED)

    next_wide = jnp.broadcast_to(boundary_begin(next_begin), (8, DH))
    mode[...] = next_wide

    begin_here = boundary_begin(chip_begin)[:1]
    here = as_float(chip_begin)
    floor = jnp.where(here - begin_here <= rows, 0.0, here)
    for tile in range(tiles):
        query_pos = (me * rows + tile * TILE + row_iota).astype(jnp.float32)
        begins = jnp.maximum(doc_begins(query_pos), floor)
        key_pos = (chip_begin - rows + lax.broadcasted_iota(jnp.int32, (TILE, 3 * rows), 1)).astype(jnp.float32)
        visible = (key_pos >= begins) & (key_pos <= query_pos)
        bias[pl.ds(tile * TILE, TILE), :] = jnp.where(visible, 0.0, MASKED)

    diagonal = lax.broadcasted_iota(jnp.int32, (TILE, TILE), 0) == lax.broadcasted_iota(
        jnp.int32, (TILE, TILE), 1
    )

    def stack(queries):
        return jnp.concatenate([queries[:, g * DH : (g + 1) * DH] for g in range(GROUPS)], axis=0)

    def raw_scores(queries, head, begin, count):
        keys = held[head, 0, pl.ds(begin, count), :]
        return lax.dot_general(
            stack(queries), keys, (((1,), (1,)), ((), ())), preferred_element_type=jnp.float32
        )

    def masked_scores(raw, mask):
        return raw.reshape(GROUPS, TILE, raw.shape[-1]) * exponent_scale + mask[None]

    def weigh(scores, highest, head, begin):
        count = scores.shape[-1]
        weights = jnp.exp2(scores - highest).astype(jnp.bfloat16).reshape(STACK, count)
        values = jnp.concatenate([held[head, 1, pl.ds(begin, count), :], ones[pl.ds(0, count), :]], axis=1)
        both = jnp.dot(weights, values, preferred_element_type=jnp.float32).reshape(GROUPS, TILE, 2 * DH)
        return both[:, :, :DH], both[:, :, DH:]

    def back_scores(step, head, tile):
        begin = rows + tile * TILE
        return raw_scores(query_back[step, pl.ds(tile * TILE, TILE), :], head, begin, 3 * rows - begin)

    def back_finish(step, head, tile, raw):
        begin = rows + tile * TILE
        span = pl.ds(tile * TILE, TILE)
        scores = masked_scores(raw, back_bias[span, pl.ds(tile * TILE, 2 * rows - tile * TILE)])
        highest = jnp.max(scores, axis=-1, keepdims=True)
        mixed, totals = weigh(scores, highest, head, begin)
        mixed = mixed * (1.0 / totals)
        level = highest + jnp.log2(totals)
        next_keys = as_float(next_begin) - mode[:1, :] <= rows
        for g in range(GROUPS):
            kept = held[head, g, pl.ds(2 * rows + tile * TILE, TILE), :].astype(jnp.float32)
            slot[step, g, span, :] = jnp.where(next_keys, kept, mixed[g]).astype(jnp.bfloat16)
            row = jnp.sum(jnp.where(diagonal, level[g], 0.0), axis=0, keepdims=True)
            stat_out[step, pl.ds(tile * GROUPS + g, 1), :] = jnp.where(next_keys, MASKED, row)

    def part_extent(side, tile):
        return rows, side * rows + (tile + 1) * TILE

    def part_scores(side, head, tile):
        return raw_scores(query_held[head, pl.ds(tile * TILE, TILE), :], head, *part_extent(side, tile))

    def part_finish(side, head, tile, raw):
        begin, count = part_extent(side, tile)
        span = pl.ds(tile * TILE, TILE)
        scores = masked_scores(raw, bias[span, pl.ds(begin, count)])
        highest = jnp.max(scores, axis=-1, keepdims=True)
        mixed, totals = weigh(scores, highest, head, begin)
        for g in range(GROUPS):
            part_mixed[head, g, span, :] = mixed[g]
            part_total[head, g, span, :] = totals[g]
            part_high[head, g, span, :] = jnp.broadcast_to(highest[g], (TILE, DH))

    def rest_extent(side, tile):
        begin = side * tile * TILE
        return begin, rows - begin

    def rest_scores(side, head, tile):
        return raw_scores(query_held[head, pl.ds(tile * TILE, TILE), :], head, *rest_extent(side, tile))

    def rest_finish(side, head, tile, raw):
        begin, count = rest_extent(side, tile)
        span = pl.ds(tile * TILE, TILE)
        scores = masked_scores(raw, bias[span, pl.ds(begin, count)])
        before = part_high[head, :, span, :]
        top = jnp.maximum(before, jnp.max(scores, axis=-1, keepdims=True))
        if side == 0:
            levels = []
            for g in range(GROUPS):
                row = stat_in[head, pl.ds(tile * GROUPS + g, 1), :]
                levels.append(jnp.sum(jnp.where(diagonal, row, 0.0), axis=1, keepdims=True))
            level = jnp.stack(levels)
            top = jnp.maximum(top, level)
        mixed, totals = weigh(scores, top[:, :, :1], head, begin)
        scale = jnp.exp2(before - top)
        mixed = mixed + part_mixed[head, :, span, :] * scale
        totals = totals + part_total[head, :, span, :] * scale
        if side == 0:
            there = jnp.exp2(level - top)
            mixed = mixed + held[head, :, span, :].astype(jnp.float32) * there
            totals = totals + there
        both = (mixed * (1.0 / totals)).astype(jnp.bfloat16)
        for g in range(GROUPS):
            out_held[head, span, pl.ds(g * DH, DH)] = both[g]

    def rest(side, head):
        raw = rest_scores(side, head, 0)
        for tile in range(tiles):
            later = rest_scores(side, head, tile + 1) if tile + 1 < tiles else None
            rest_finish(side, head, tile, raw)
            raw = later
        out_store(head).start()

    def wait_direct(side, step):
        @pl.when(has_prev)
        def _():
            slot_to_next(step, received).wait_recv()
            relay(step, side).start()
            if side == 0:
                stat_to_next(step, step).wait_recv()

    def wait_relayed(side, step):
        @pl.when(has_prev)
        def _():
            relay(step, 1 - side).wait_recv()
            if side == 0:
                stat_to_next(step, SPLIT + step).wait_recv()

    def run(side):
        @pl.loop(0, HK if side else SPLIT)
        def _(head):
            from_core(head).wait_recv()

        @pl.loop(0, SPLIT)
        def _(step):
            head = side * SPLIT + step
            for tile in range(tiles):
                @pl.when(has_next)
                def _():
                    query_to_prev(step, 0, tile).wait_recv()

                raw_back = back_scores(step, head, tile)
                raw_first = part_scores(side, step, tile)
                back_finish(step, head, tile, raw_back)

                @pl.when(has_next)
                def _():
                    slot_to_next(step, pl.ds(tile * TILE, TILE)).start()
                    if tile == tiles - 1:
                        stat_to_next(step, head).start()

                raw_second = part_scores(side, SPLIT + step, tile)
                part_finish(side, step, tile, raw_first)
                part_finish(side, SPLIT + step, tile, raw_second)

                if tile == tiles - 2:
                    @pl.when(step >= 1)
                    def _():
                        wait_direct(side, step - 1)

            @pl.when(step >= 1)
            def _():
                rest(side, side * SPLIT + step - 1)
                wait_relayed(side, step - 1)
                rest(side, (1 - side) * SPLIT + step - 1)

        wait_direct(side, SPLIT - 1)
        rest(side, side * SPLIT + SPLIT - 1)
        wait_relayed(side, SPLIT - 1)
        rest(side, (1 - side) * SPLIT + SPLIT - 1)

    @pl.when(even)
    def _():
        run(0)

    @pl.when(odd)
    def _():
        run(1)

    @pl.loop(0, HK)
    def _(head):
        out_store(head).wait()

        @pl.when(jnp.logical_or(even, head < SPLIT))
        def _():
            to_core(head).wait_send()

    @pl.loop(0, SPLIT)
    def _(step):
        @pl.when(has_next)
        def _():
            slot_to_next(step, received).wait_send()
            stat_to_next(step, step).wait_send()

        @pl.when(has_prev)
        def _():
            relay(step, core).wait_send()

            @pl.when(even)
            def _():
                for side in range(2):
                    query_sent(side * SPLIT + step).wait_send()


def on_device(queries, keys, values, doc_lengths):
    rows = keys.shape[0]
    docs = doc_lengths.shape[0]
    shards = lax.axis_size("cp")
    stats = rows // TILE * GROUPS
    dma = pltpu.SemaphoreType.DMA
    hbm = pl.BlockSpec(memory_space=pl.ANY)
    return pl.pallas_call(
        functools.partial(kernel, shards),
        out_shape=jax.ShapeDtypeStruct(queries.shape, queries.dtype),
        in_specs=[hbm] * 4,
        out_specs=hbm,
        scratch_shapes=[
            pltpu.VMEM((HK, 2, 3 * rows, DH), keys.dtype),
            pltpu.VMEM((HK, rows, WIDTH), queries.dtype),
            pltpu.VMEM((HK, rows, WIDTH), queries.dtype),
            pltpu.VMEM((SPLIT, rows, WIDTH), queries.dtype),
            pltpu.VMEM((SPLIT, 2, rows, DH), keys.dtype),
            pltpu.VMEM((SPLIT, stats, TILE), jnp.float32),
            pltpu.VMEM((HK, stats, TILE), jnp.float32),
            pltpu.VMEM((rows, 3 * rows), jnp.float32),
            pltpu.VMEM((rows, 2 * rows), jnp.float32),
            pltpu.VMEM((1, docs), jnp.int32),
            pltpu.VMEM((8, DH), jnp.float32),
            pltpu.VMEM((2 * rows, DH), keys.dtype),
            pltpu.VMEM((HK, GROUPS, rows, DH), jnp.float32),
            pltpu.VMEM((HK, GROUPS, rows, DH), jnp.float32),
            pltpu.VMEM((HK, GROUPS, rows, DH), jnp.float32),
            dma,
            dma((HK, 2)),
            dma((HK,)),
            dma((HK,)),
            dma((HK,)),
            dma((HK,)),
            dma((HK,)),
            dma((SPLIT, rows // TILE)),
            dma((SPLIT,)),
            dma((SPLIT,)),
            dma((SPLIT,)),
            dma((SPLIT,)),
            dma((SPLIT,)),
            dma((HK,)),
        ],
        compiler_params=pltpu.CompilerParams(
            collective_id=0, has_side_effects=True, vmem_limit_bytes=58 * 1024 * 1024
        ),
    )(doc_lengths.reshape(1, docs), queries, keys, values)


def solution(mesh):
    return jax.shard_map(
        on_device,
        mesh=mesh,
        in_specs=(P(("grp", "cp"), None), P(("grp", "cp"), None), P(("grp", "cp"), None), P("grp")),
        out_specs=P(("grp", "cp"), None),
        check_vma=False,
    )
```

```python
import functools
import math

import jax
import jax.numpy as jnp
from jax import lax
from jax.experimental import pallas as pl
from jax.experimental.pallas import tpu as pltpu
from jax.sharding import PartitionSpec as P

HQ = 16
HK = 8
DH = 128
GROUPS = HQ // HK
WIDTH = GROUPS * DH
TILE = 128
STACK = GROUPS * TILE
MASKED = -1e30
SPLIT = HK // 2
MESH = pl.DeviceIdType.MESH

LOG2E = math.log2(math.e)
exponent_scale = 144.0 ** (-0.5) * LOG2E


def kernel(
    shards,
    lengths_ref,
    queries_ref,
    keys_ref,
    values_ref,
    out_ref,
    held,
    query_held,
    query_back,
    query_extra,
    slot,
    slot_extra,
    stat_out,
    stat_in,
    stat_extra_out,
    stat_extra_in,
    bias,
    back_bias,
    lengths,
    mode,
    ones,
    part_mixed,
    part_total,
    part_high,
    lengths_sem,
    load_sem,
    query_sem,
    core_send,
    core_recv,
    query_send,
    query_recv,
    extra_recv,
    extra_send,
    extra_stat_send,
    extra_stat_recv,
    slot_send,
    slot_recv,
    relay_send,
    relay_recv,
    stat_send,
    stat_recv,
):
    me = lax.axis_index("cp")
    core = lax.rem(me, 2)
    even = core == 0
    odd = core == 1
    partner = me + 1 - 2 * core
    rows = keys_ref.shape[0]
    docs = lengths_ref.shape[1]
    tiles = rows // TILE
    received = pl.ds(0, rows)
    own = pl.ds(pl.multiple_of((1 + core) * rows, rows), rows)
    has_prev = me >= 2
    has_next = me < shards - 2
    chip_begin = (me - core) * rows
    next_begin = chip_begin + 2 * rows

    def loads(head):
        lanes = pl.ds(pl.multiple_of(head * DH, DH), DH)
        return (
            pltpu.make_async_copy(keys_ref.at[:, lanes], held.at[head, 0, own], load_sem.at[head, 0]),
            pltpu.make_async_copy(values_ref.at[:, lanes], held.at[head, 1, own], load_sem.at[head, 1]),
        )

    def in_turn(turn):
        return lax.rem(turn, 2) * SPLIT + turn // 2

    def query_load(head):
        lanes = pl.ds(pl.multiple_of(head * WIDTH, WIDTH), WIDTH)
        return pltpu.make_async_copy(queries_ref.at[:, lanes], query_held.at[head], query_sem.at[head])

    def remote(source, target, send, recv, device):
        return pltpu.make_async_remote_copy(
            src_ref=source,
            dst_ref=target,
            send_sem=send,
            recv_sem=recv,
            device_id={"cp": device},
            device_id_type=MESH,
        )

    def to_core(head):
        return remote(held.at[head, :, own], held.at[head, :, own], core_send.at[head], core_recv.at[head], partner)

    def from_core(head):
        other = pl.ds(pl.multiple_of((2 - core) * rows, rows), rows)
        return remote(held.at[head, :, other], held.at[head, :, other], core_send.at[head], core_recv.at[head], partner)

    def query_to_prev(step, side, tile):
        span = pl.ds(tile * TILE, TILE)
        return remote(
            query_held.at[side * SPLIT + step, span],
            query_back.at[step, span],
            query_send.at[side * SPLIT + step],
            query_recv.at[step, tile],
            me - 2 + side,
        )

    def extra_query(step):
        return remote(
            query_held.at[SPLIT + step, pl.ds(0, TILE)],
            query_extra.at[step],
            query_send.at[SPLIT + step],
            extra_recv.at[step],
            me - 2,
        )

    def extra_slot(step):
        return remote(
            slot_extra.at[step],
            held.at[SPLIT + step, :, pl.ds(0, TILE)],
            extra_send.at[step],
            slot_recv.at[step],
            me + 3,
        )

    def extra_stat(step):
        return remote(
            stat_extra_out.at[step],
            stat_extra_in.at[step],
            extra_stat_send.at[step],
            extra_stat_recv.at[step],
            me + 2,
        )

    def query_sent(head):
        return remote(
            query_held.at[head], query_held.at[head], query_send.at[head], query_send.at[head], me - 2
        )

    def slot_to_next(step, span):
        return remote(
            slot.at[step, :, span],
            held.at[core * SPLIT + step, :, span],
            slot_send.at[step],
            slot_recv.at[step],
            me + 2,
        )

    def relay(step, side):
        head = side * SPLIT + step
        return remote(
            held.at[head, :, received], held.at[head, :, received], relay_send.at[step], relay_recv.at[step], partner
        )

    def stat_to_next(step, head):
        return remote(
            stat_out.at[step], stat_in.at[head], stat_send.at[step], stat_recv.at[head], me + 2 - core
        )

    barrier = pltpu.get_barrier_semaphore()

    def greet(device):
        pl.semaphore_signal(barrier, inc=1, device_id={"cp": device}, device_id_type=MESH)

    greet(partner)

    @pl.when(has_prev)
    def _():
        greet(me - core - 2)
        greet(me - core - 1)

    @pl.when(has_next)
    def _():
        greet(me - core + 2)
        greet(me - core + 3)

    @pl.loop(0, SPLIT)
    def _(step):
        query_load(step).start()
        query_load(SPLIT + step).start()

    lengths_load = pltpu.make_async_copy(lengths_ref, lengths, lengths_sem)
    lengths_load.start()

    @pl.loop(0, HK)
    def _(turn):
        for copy in loads(in_turn(turn)):
            copy.start()

    back_peers = jnp.where(has_prev, 2, 0)
    next_peers = jnp.where(has_next, 2, 0)
    pl.semaphore_wait(barrier, 1 + back_peers + next_peers)

    @pl.loop(0, SPLIT)
    def _(step):
        query_load(step).wait()
        query_load(SPLIT + step).wait()

        @pl.when(jnp.logical_and(even, has_prev))
        def _():
            for tile in range(tiles):
                query_to_prev(step, 0, tile).start()
                if tile == 0:
                    extra_query(step).start()
                else:
                    query_to_prev(step, 1, tile).start()

    @pl.loop(0, HK)
    def _(turn):
        head = in_turn(turn)
        for copy in loads(head):
            copy.wait()

        to_core(head).start()

    @pl.when(jnp.logical_not(has_prev))
    def _():
        held[:, :, received, :] = jnp.zeros((HK, 2, rows, DH), held.dtype)

        @pl.when(even)
        def _():
            stat_in[...] = jnp.full(stat_in.shape, MASKED, jnp.float32)
            stat_extra_in[...] = jnp.full(stat_extra_in.shape, MASKED, jnp.float32)

    ones[...] = jnp.ones(ones.shape, ones.dtype)
    stat_out[...] = jnp.full(stat_out.shape, MASKED, jnp.float32)
    stat_extra_out[...] = jnp.full(stat_extra_out.shape, MASKED, jnp.float32)

    lengths_load.wait()
    doc_row = lax.broadcasted_iota(jnp.int32, (docs, docs), 0)
    doc_lane = lax.broadcasted_iota(jnp.int32, (docs, docs), 1)
    length_row = lengths[...].astype(jnp.float32)
    length_column = jnp.sum(jnp.where(doc_row == doc_lane, length_row, 0.0), axis=1, keepdims=True)
    doc_ends = jnp.sum(jnp.where(doc_row <= doc_lane, length_column, 0.0), axis=0, keepdims=True)

    def doc_begins(positions):
        return jnp.max(jnp.where(positions >= doc_ends, doc_ends, 0.0), axis=1, keepdims=True)

    def boundary_begin(boundary):
        return doc_begins(jnp.full((8, 1), boundary, jnp.int32).astype(jnp.float32))

    def as_float(number):
        return jnp.full((1, 1), number, jnp.int32).astype(jnp.float32)

    row_iota = lax.broadcasted_iota(jnp.int32, (TILE, 1), 0)
    for tile in range(tiles):
        begins = doc_begins((next_begin + tile * TILE + row_iota).astype(jnp.float32))
        key_pos = (chip_begin + lax.broadcasted_iota(jnp.int32, (TILE, 2 * rows), 1)).astype(jnp.float32)
        back_bias[pl.ds(tile * TILE, TILE), :] = jnp.where(key_pos >= begins, 0.0, MASKED)

    next_wide = jnp.broadcast_to(boundary_begin(next_begin), (8, DH))
    mode[...] = next_wide

    begin_here = boundary_begin(chip_begin)[:1]
    here = as_float(chip_begin)
    floor = jnp.where(here - begin_here <= rows, 0.0, here)
    for tile in range(tiles):
        query_pos = (me * rows + tile * TILE + row_iota).astype(jnp.float32)
        begins = jnp.maximum(doc_begins(query_pos), floor)
        key_pos = (chip_begin - rows + lax.broadcasted_iota(jnp.int32, (TILE, 3 * rows), 1)).astype(jnp.float32)
        visible = (key_pos >= begins) & (key_pos <= query_pos)
        bias[pl.ds(tile * TILE, TILE), :] = jnp.where(visible, 0.0, MASKED)

    diagonal = lax.broadcasted_iota(jnp.int32, (TILE, TILE), 0) == lax.broadcasted_iota(
        jnp.int32, (TILE, TILE), 1
    )

    def stack(queries):
        return jnp.concatenate([queries[:, g * DH : (g + 1) * DH] for g in range(GROUPS)], axis=0)

    def raw_scores(queries, head, begin, count):
        keys = held[head, 0, pl.ds(begin, count), :]
        return lax.dot_general(
            stack(queries), keys, (((1,), (1,)), ((), ())), preferred_element_type=jnp.float32
        )

    def masked_scores(raw, mask):
        return raw.reshape(GROUPS, TILE, raw.shape[-1]) * exponent_scale + mask[None]

    def weigh(scores, highest, head, begin):
        count = scores.shape[-1]
        weights = jnp.exp2(scores - highest).astype(jnp.bfloat16).reshape(STACK, count)
        values = jnp.concatenate([held[head, 1, pl.ds(begin, count), :], ones[pl.ds(0, count), :]], axis=1)
        both = jnp.dot(weights, values, preferred_element_type=jnp.float32).reshape(GROUPS, TILE, 2 * DH)
        return both[:, :, :DH], both[:, :, DH:]

    def back_scores(step, head, tile, extra):
        begin = rows + tile * TILE
        queries = query_extra[step] if extra else query_back[step, pl.ds(tile * TILE, TILE), :]
        return raw_scores(queries, head, begin, 3 * rows - begin)

    def back_finish(step, head, tile, extra, raw):
        begin = rows + tile * TILE
        span = pl.ds(tile * TILE, TILE)
        scores = masked_scores(raw, back_bias[span, pl.ds(tile * TILE, 2 * rows - tile * TILE)])
        highest = jnp.max(scores, axis=-1, keepdims=True)
        mixed, totals = weigh(scores, highest, head, begin)
        mixed = mixed * (1.0 / totals)
        level = highest + jnp.log2(totals)
        next_keys = as_float(next_begin) - mode[:1, :] <= rows
        for g in range(GROUPS):
            kept = held[head, g, pl.ds(2 * rows + tile * TILE, TILE), :].astype(jnp.float32)
            sent = jnp.where(next_keys, kept, mixed[g]).astype(jnp.bfloat16)
            row = jnp.sum(jnp.where(diagonal, level[g], 0.0), axis=0, keepdims=True)
            row = jnp.where(next_keys, MASKED, row)
            if extra:
                slot_extra[step, g] = sent
                stat_extra_out[step, pl.ds(g, 1), :] = row
            else:
                slot[step, g, span, :] = sent
                stat_out[step, pl.ds(tile * GROUPS + g, 1), :] = row

    def part_extent(side, tile):
        return rows, side * rows + (tile + 1) * TILE

    def part_scores(side, head, tile):
        return raw_scores(query_held[head, pl.ds(tile * TILE, TILE), :], head, *part_extent(side, tile))

    def part_finish(side, head, tile, raw):
        begin, count = part_extent(side, tile)
        span = pl.ds(tile * TILE, TILE)
        scores = masked_scores(raw, bias[span, pl.ds(begin, count)])
        highest = jnp.max(scores, axis=-1, keepdims=True)
        mixed, totals = weigh(scores, highest, head, begin)
        for g in range(GROUPS):
            part_mixed[head, g, span, :] = mixed[g]
            part_total[head, g, span, :] = totals[g]
            part_high[head, g, span, :] = jnp.broadcast_to(highest[g], (TILE, DH))

    def rest_extent(side, tile):
        begin = side * tile * TILE
        return begin, rows - begin

    def rest_scores(side, head, step, tile):
        return raw_scores(query_held[head, pl.ds(tile * TILE, TILE), :], head, *rest_extent(side, tile))

    def rest_finish(side, head, step, tile, raw):
        begin, count = rest_extent(side, tile)
        span = pl.ds(tile * TILE, TILE)
        scores = masked_scores(raw, bias[span, pl.ds(begin, count)])
        tops, levels = [], []
        for g in range(GROUPS):
            top = jnp.maximum(part_high[head, g, span, :], jnp.max(scores[g], axis=-1, keepdims=True))
            if side == 0:
                if step is not None and tile == 0:
                    row = stat_extra_in[step, pl.ds(g, 1), :]
                else:
                    row = stat_in[head, pl.ds(tile * GROUPS + g, 1), :]
                level = jnp.sum(jnp.where(diagonal, row, 0.0), axis=1, keepdims=True)
                top = jnp.maximum(top, level)
                levels.append(level)
            tops.append(top)
        wide = jnp.stack([jnp.concatenate([top] * (count // DH), axis=1) for top in tops])
        all_mixed, all_totals = weigh(scores, wide, head, begin)
        for g in range(GROUPS):
            scale = jnp.exp2(part_high[head, g, span, :] - tops[g])
            mixed = all_mixed[g] + part_mixed[head, g, span, :] * scale
            totals = all_totals[g] + part_total[head, g, span, :] * scale
            if side == 0:
                there = jnp.exp2(levels[g] - tops[g])
                mixed = mixed + held[head, g, span, :].astype(jnp.float32) * there
                totals = totals + there
            out_ref[span, pl.ds(pl.multiple_of(head * WIDTH, WIDTH) + g * DH, DH)] = (mixed * (1.0 / totals)).astype(jnp.bfloat16)

    def pipelined(jobs):
        raw = jobs[0][0](*jobs[0][2])
        for at, (_, finish, job) in enumerate(jobs):
            later = None
            if at + 1 < len(jobs):
                later = jobs[at + 1][0](*jobs[at + 1][2])
            finish(*job, raw)
            raw = later

    def back(side, step, tile):
        return back_scores, back_finish, (step, side * SPLIT + step, tile, False)

    def back_extra(step):
        return back_scores, back_finish, (step, SPLIT + step, 0, True)

    def part(side, head, tile):
        return part_scores, part_finish, (side, head, tile)

    def rest(side, step, at):
        extra = step if at == 1 else None
        pipelined([(rest_scores, rest_finish, (side, at * SPLIT + step, extra, tile)) for tile in range(tiles)])

    def wait_direct(side, step):
        @pl.when(has_prev)
        def _():
            slot_to_next(step, received).wait_recv()
            relay(step, side).start()
            if side == 0:
                stat_to_next(step, step).wait_recv()

    def wait_relayed(side, step):
        @pl.when(has_prev)
        def _():
            relay(step, 1 - side).wait_recv()
            if side == 0:
                stat_to_next(step, SPLIT + step).wait_recv()
                extra_stat(step).wait_recv()

    def wait_query(side, step, tile):
        @pl.when(has_next)
        def _():
            query_to_prev(step, 0, tile).wait_recv()
            if side == 0 and tile == 1:
                extra_query(step).wait_recv()

    def send_slot(side, step, tile):
        @pl.when(has_next)
        def _():
            slot_to_next(step, pl.ds(tile * TILE, TILE)).start()
            if side == 0 and tile == 1:
                extra_slot(step).start()
                extra_stat(step).start()
            if tile == tiles - 1:
                stat_to_next(step, side * SPLIT + step).start()

    def run(side):
        last = SPLIT - 1
        first = side
        from_core(0).wait_recv()
        from_core(SPLIT).wait_recv()
        pipelined([part(side, head, tile) for head in (0, SPLIT) for tile in range(tiles)])

        def backs(step, tile):
            jobs = [back(side, step, tile)]
            return [back_extra(step)] + jobs if side == 0 and tile == 1 else jobs

        @pl.loop(0, last)
        def _(step):
            from_core(step + 1).wait_recv()
            from_core(SPLIT + step + 1).wait_recv()
            for tile in range(first, tiles):
                wait_query(side, step, tile)
                jobs = backs(step, tile)
                for at in range(0 if tile == first else tile, tile + 1):
                    jobs.append(part(side, step + 1, at))
                    jobs.append(part(side, SPLIT + step + 1, at))
                pipelined(jobs)
                send_slot(side, step, tile)
                if tile == first:

                    @pl.when(step >= 2)
                    def _():
                        wait_direct(side, step - 2)

            @pl.when(step >= 2)
            def _():
                rest(side, step - 2, side)
                wait_relayed(side, step - 2)
                rest(side, step - 2, 1 - side)

        for tile in range(first, tiles):
            wait_query(side, last, tile)
            pipelined(backs(last, tile))
            send_slot(side, last, tile)
            if tile == first:
                wait_direct(side, last - 2)

        wait_direct(side, last - 1)
        rest(side, last - 2, side)
        wait_relayed(side, last - 2)
        rest(side, last - 2, 1 - side)
        rest(side, last - 1, side)
        wait_relayed(side, last - 1)
        rest(side, last - 1, 1 - side)
        wait_direct(side, last)
        rest(side, last, side)
        wait_relayed(side, last)
        rest(side, last, 1 - side)

    @pl.when(even)
    def _():
        run(0)

    @pl.when(odd)
    def _():
        run(1)

    @pl.loop(0, HK)
    def _(head):
        to_core(head).wait_send()

    @pl.loop(0, SPLIT)
    def _(step):
        @pl.when(has_next)
        def _():
            stat_to_next(step, step).wait_send()

            @pl.when(even)
            def _():
                slot_to_next(step, received).wait_send()
                extra_slot(step).wait_send()
                extra_stat(step).wait_send()

            @pl.when(odd)
            def _():
                slot_to_next(step, pl.ds(TILE, rows - TILE)).wait_send()

        @pl.when(has_prev)
        def _():
            relay(step, core).wait_send()

            @pl.when(even)
            def _():
                for side in range(2):
                    query_sent(side * SPLIT + step).wait_send()


def on_device(queries, keys, values, doc_lengths):
    rows = keys.shape[0]
    docs = doc_lengths.shape[0]
    shards = lax.axis_size("cp")
    stats = rows // TILE * GROUPS
    dma = pltpu.SemaphoreType.DMA
    hbm = pl.BlockSpec(memory_space=pltpu.HBM)
    return pl.pallas_call(
        functools.partial(kernel, shards),
        out_shape=pltpu.VMEM(queries.shape, queries.dtype),
        in_specs=[hbm] * 4,
        out_specs=pl.BlockSpec(memory_space=pltpu.VMEM),
        scratch_shapes=[
            pltpu.VMEM((HK, 2, 3 * rows, DH), keys.dtype),
            pltpu.VMEM((HK, rows, WIDTH), queries.dtype),
            pltpu.VMEM((SPLIT, rows, WIDTH), queries.dtype),
            pltpu.VMEM((SPLIT, TILE, WIDTH), queries.dtype),
            pltpu.VMEM((SPLIT, 2, rows, DH), keys.dtype),
            pltpu.VMEM((SPLIT, 2, TILE, DH), keys.dtype),
            pltpu.VMEM((SPLIT, stats, TILE), jnp.float32),
            pltpu.VMEM((HK, stats, TILE), jnp.float32),
            pltpu.VMEM((SPLIT, 8, TILE), jnp.float32),
            pltpu.VMEM((SPLIT, 8, TILE), jnp.float32),
            pltpu.VMEM((rows, 3 * rows), jnp.float32),
            pltpu.VMEM((rows, 2 * rows), jnp.float32),
            pltpu.VMEM((1, docs), jnp.int32),
            pltpu.VMEM((8, DH), jnp.float32),
            pltpu.VMEM((2 * rows, DH), keys.dtype),
            pltpu.VMEM((HK, GROUPS, rows, DH), jnp.float32),
            pltpu.VMEM((HK, GROUPS, rows, DH), jnp.float32),
            pltpu.VMEM((HK, GROUPS, rows, DH), jnp.float32),
            dma,
            dma((HK, 2)),
            dma((HK,)),
            dma((HK,)),
            dma((HK,)),
            dma((HK,)),
            dma((SPLIT, rows // TILE)),
            dma((SPLIT,)),
            dma((SPLIT,)),
            dma((SPLIT,)),
            dma((SPLIT,)),
            dma((SPLIT,)),
            dma((SPLIT,)),
            dma((SPLIT,)),
            dma((SPLIT,)),
            dma((SPLIT,)),
            dma((HK,)),
        ],
        compiler_params=pltpu.CompilerParams(
            collective_id=0, has_side_effects=True, vmem_limit_bytes=50 * 1024 * 1024
        ),
    )(*(pltpu.with_memory_space_constraint(x, pltpu.HBM) for x in (doc_lengths.reshape(1, docs), queries, keys, values)))


def solution(mesh):
    return jax.shard_map(
        on_device,
        mesh=mesh,
        in_specs=(P(("grp", "cp"), None), P(("grp", "cp"), None), P(("grp", "cp"), None), P("grp")),
        out_specs=P(("grp", "cp"), None),
        check_vma=False,
    )
```

```python
import functools
import math

import jax
import jax.numpy as jnp
from jax import lax
from jax.experimental import pallas as pl
from jax.experimental.pallas import tpu as pltpu
from jax.sharding import PartitionSpec as P

HQ = 16
HK = 8
DH = 128
GROUPS = HQ // HK
WIDTH = GROUPS * DH
TILE = 128
STACK = GROUPS * TILE
MASKED = -1e30
SPLIT = HK // 2
FORWARD = HK - 1
MESH = pl.DeviceIdType.MESH

LOG2E = math.log2(math.e)
exponent_scale = 144.0 ** (-0.5) * LOG2E


def kernel(
    shards,
    lengths_ref,
    queries_ref,
    keys_ref,
    values_ref,
    out_ref,
    held,
    query_held,
    query_back,
    far_held,
    slot,
    stat_out,
    stat_in,
    bias,
    back_bias,
    far_bias,
    lengths,
    mode,
    ones,
    part_mixed,
    part_total,
    part_high,
    lengths_sem,
    far_send,
    far_recv,
    load_sem,
    query_sem,
    core_send,
    core_recv,
    query_send,
    query_recv,
    slot_send,
    slot_recv,
    relay_send,
    relay_recv,
    stat_send,
    stat_recv,
):
    me = lax.axis_index("cp")
    core = lax.rem(me, 2)
    even = core == 0
    odd = core == 1
    partner = me + 1 - 2 * core
    rows = keys_ref.shape[0]
    docs = lengths_ref.shape[1]
    tiles = rows // TILE
    received = pl.ds(0, rows)
    own = pl.ds(pl.multiple_of((1 + core) * rows, rows), rows)
    has_prev = me >= 2
    has_next = me < shards - 2
    chip_begin = (me - core) * rows
    next_begin = chip_begin + 2 * rows

    def loads(head):
        lanes = pl.ds(pl.multiple_of(head * DH, DH), DH)
        return (
            pltpu.make_async_copy(keys_ref.at[:, lanes], held.at[head, 0, own], load_sem.at[head, 0]),
            pltpu.make_async_copy(values_ref.at[:, lanes], held.at[head, 1, own], load_sem.at[head, 1]),
        )

    def in_turn(turn):
        order = lax.rem(turn + HK - 1, HK)
        return lax.rem(order, 2) * SPLIT + order // 2

    def query_load(head):
        lanes = pl.ds(pl.multiple_of(head * WIDTH, WIDTH), WIDTH)
        return pltpu.make_async_copy(queries_ref.at[:, lanes], query_held.at[head], query_sem.at[head])

    def remote(source, target, send, recv, device):
        return pltpu.make_async_remote_copy(
            src_ref=source,
            dst_ref=target,
            send_sem=send,
            recv_sem=recv,
            device_id={"cp": device},
            device_id_type=MESH,
        )

    def to_core(head):
        return remote(held.at[head, :, own], held.at[head, :, own], core_send.at[head], core_recv.at[head], partner)

    def from_core(head):
        other = pl.ds(pl.multiple_of((2 - core) * rows, rows), rows)
        return remote(held.at[head, :, other], held.at[head, :, other], core_send.at[head], core_recv.at[head], partner)

    def query_to_prev(step, side, tile):
        span = pl.ds(tile * TILE, TILE)
        return remote(
            query_held.at[side * SPLIT + step, span],
            query_back.at[step, span],
            query_send.at[side * SPLIT + step],
            query_recv.at[step, tile],
            me - 2 + side,
        )

    def far_to_next():
        return remote(held.at[FORWARD, :, own], far_held, far_send, far_recv, me + 2)

    def near_to_next():
        return remote(
            held.at[FORWARD, :, own],
            held.at[FORWARD, :, received],
            slot_send.at[SPLIT - 1],
            slot_recv.at[SPLIT - 1],
            me + 2,
        )

    def query_sent(head):
        return remote(
            query_held.at[head], query_held.at[head], query_send.at[head], query_send.at[head], me - 2
        )

    def arrival(step, tile):
        return step + tile if step is SPLIT - 1 else step

    def slot_to_next(step, span, tile=0):
        return remote(
            slot.at[step, :, span],
            held.at[core * SPLIT + step, :, span],
            slot_send.at[step],
            slot_recv.at[arrival(step, tile)],
            me + 2,
        )

    def relay(step, side, span=received):
        head = side * SPLIT + step
        return remote(
            held.at[head, :, span], held.at[head, :, span], relay_send.at[step], relay_recv.at[step], partner
        )

    def stat_to_next(step, head):
        return remote(
            stat_out.at[step], stat_in.at[head], stat_send.at[step], stat_recv.at[head], me + 2 - core
        )

    barrier = pltpu.get_barrier_semaphore()

    def greet(device):
        pl.semaphore_signal(barrier, inc=1, device_id={"cp": device}, device_id_type=MESH)

    greet(partner)

    @pl.when(has_prev)
    def _():
        greet(me - core - 2)
        greet(me - core - 1)

    @pl.when(has_next)
    def _():
        greet(me - core + 2)
        greet(me - core + 3)

    @pl.loop(0, SPLIT)
    def _(step):
        query_load(step).start()
        query_load(SPLIT + step).start()

    lengths_load = pltpu.make_async_copy(lengths_ref, lengths, lengths_sem)
    lengths_load.start()

    @pl.loop(0, HK)
    def _(turn):
        for copy in loads(in_turn(turn)):
            copy.start()

    back_peers = jnp.where(has_prev, 2, 0)
    next_peers = jnp.where(has_next, 2, 0)
    pl.semaphore_wait(barrier, 1 + back_peers + next_peers)

    @pl.loop(0, SPLIT)
    def _(step):
        query_load(step).wait()
        query_load(SPLIT + step).wait()

        @pl.when(jnp.logical_and(even, has_prev))
        def _():
            for tile in range(tiles):
                query_to_prev(step, 0, tile).start()

                @pl.when(step < SPLIT - 1)
                def _():
                    query_to_prev(step, 1, tile).start()

    @pl.loop(0, HK)
    def _(turn):
        head = in_turn(turn)
        for copy in loads(head):
            copy.wait()

        @pl.when(jnp.logical_and(has_next, turn == 0))
        def _():
            @pl.when(even)
            def _():
                far_to_next().start()

            @pl.when(odd)
            def _():
                near_to_next().start()

        to_core(head).start()

    @pl.when(jnp.logical_not(has_prev))
    def _():
        held[:, :, received, :] = jnp.zeros((HK, 2, rows, DH), held.dtype)

        @pl.when(even)
        def _():
            far_held[...] = jnp.zeros(far_held.shape, far_held.dtype)
            stat_in[...] = jnp.full(stat_in.shape, MASKED, jnp.float32)

    ones[...] = jnp.ones(ones.shape, ones.dtype)
    stat_out[...] = jnp.full(stat_out.shape, MASKED, jnp.float32)

    lengths_load.wait()
    doc_row = lax.broadcasted_iota(jnp.int32, (docs, docs), 0)
    doc_lane = lax.broadcasted_iota(jnp.int32, (docs, docs), 1)
    length_row = lengths[...].astype(jnp.float32)
    length_column = jnp.sum(jnp.where(doc_row == doc_lane, length_row, 0.0), axis=1, keepdims=True)
    doc_ends = jnp.sum(jnp.where(doc_row <= doc_lane, length_column, 0.0), axis=0, keepdims=True)

    def doc_begins(positions):
        return jnp.max(jnp.where(positions >= doc_ends, doc_ends, 0.0), axis=1, keepdims=True)

    def boundary_begin(boundary):
        return doc_begins(jnp.full((8, 1), boundary, jnp.int32).astype(jnp.float32))

    def as_float(number):
        return jnp.full((1, 1), number, jnp.int32).astype(jnp.float32)

    row_iota = lax.broadcasted_iota(jnp.int32, (TILE, 1), 0)
    for tile in range(tiles):
        begins = doc_begins((next_begin + tile * TILE + row_iota).astype(jnp.float32))
        key_pos = (chip_begin + lax.broadcasted_iota(jnp.int32, (TILE, 2 * rows), 1)).astype(jnp.float32)
        back_bias[pl.ds(tile * TILE, TILE), :] = jnp.where(key_pos >= begins, 0.0, MASKED)

    next_wide = jnp.broadcast_to(boundary_begin(next_begin), (8, DH))
    mode[...] = next_wide

    begin_here = boundary_begin(chip_begin)[:1]
    here = as_float(chip_begin)
    floor = jnp.where(here - begin_here <= rows, 0.0, here)
    for tile in range(tiles):
        query_pos = (me * rows + tile * TILE + row_iota).astype(jnp.float32)
        begins = doc_begins(query_pos)
        far_pos = (chip_begin - 2 * rows + lax.broadcasted_iota(jnp.int32, (TILE, 2 * rows), 1)).astype(jnp.float32)
        far_bias[pl.ds(tile * TILE, TILE), :] = jnp.where(far_pos >= begins, 0.0, MASKED)
        begins = jnp.maximum(begins, floor)
        key_pos = (chip_begin - rows + lax.broadcasted_iota(jnp.int32, (TILE, 3 * rows), 1)).astype(jnp.float32)
        visible = (key_pos >= begins) & (key_pos <= query_pos)
        bias[pl.ds(tile * TILE, TILE), :] = jnp.where(visible, 0.0, MASKED)

    diagonal = lax.broadcasted_iota(jnp.int32, (TILE, TILE), 0) == lax.broadcasted_iota(
        jnp.int32, (TILE, TILE), 1
    )

    def stack(queries):
        return jnp.concatenate([queries[:, g * DH : (g + 1) * DH] for g in range(GROUPS)], axis=0)

    def dot_keys(queries, keys):
        return lax.dot_general(
            stack(queries), keys, (((1,), (1,)), ((), ())), preferred_element_type=jnp.float32
        )

    def raw_scores(queries, head, begin, count):
        return dot_keys(queries, held[head, 0, pl.ds(begin, count), :])

    def masked_scores(raw, mask):
        return raw.reshape(GROUPS, TILE, raw.shape[-1]) * exponent_scale + mask[None]

    def weigh(scores, highest, head, begin):
        return mix(scores, highest, held[head, 1, pl.ds(begin, scores.shape[-1]), :])

    def mix(scores, highest, values):
        count = scores.shape[-1]
        weights = jnp.exp2(scores - highest).astype(jnp.bfloat16).reshape(STACK, count)
        values = jnp.concatenate([values, ones[pl.ds(0, count), :]], axis=1)
        both = jnp.dot(weights, values, preferred_element_type=jnp.float32).reshape(GROUPS, TILE, 2 * DH)
        return both[:, :, :DH], both[:, :, DH:]

    def back_scores(step, head, tile):
        begin = rows + tile * TILE
        return raw_scores(query_back[step, pl.ds(tile * TILE, TILE), :], head, begin, 3 * rows - begin)

    def back_finish(step, head, tile, raw):
        begin = rows + tile * TILE
        span = pl.ds(tile * TILE, TILE)
        scores = masked_scores(raw, back_bias[span, pl.ds(tile * TILE, 2 * rows - tile * TILE)])
        highest = jnp.max(scores, axis=-1, keepdims=True)
        mixed, totals = weigh(scores, highest, head, begin)
        mixed = mixed * (1.0 / totals)
        level = highest + jnp.log2(totals)
        next_keys = as_float(next_begin) - mode[:1, :] <= rows
        for g in range(GROUPS):
            kept = held[head, g, pl.ds(2 * rows + tile * TILE, TILE), :].astype(jnp.float32)
            sent = jnp.where(next_keys, kept, mixed[g]).astype(jnp.bfloat16)
            row = jnp.sum(jnp.where(diagonal, level[g], 0.0), axis=0, keepdims=True)
            row = jnp.where(next_keys, MASKED, row)
            slot[step, g, span, :] = sent
            stat_out[step, pl.ds(tile * GROUPS + g, 1), :] = row

    def part_extent(side, tile):
        return rows, side * rows + (tile + 1) * TILE

    def part_scores(side, head, tile):
        return raw_scores(query_held[head, pl.ds(tile * TILE, TILE), :], head, *part_extent(side, tile))

    def part_finish(side, head, tile, raw):
        begin, count = part_extent(side, tile)
        span = pl.ds(tile * TILE, TILE)
        scores = masked_scores(raw, bias[span, pl.ds(begin, count)])
        highest = jnp.max(scores, axis=-1, keepdims=True)
        mixed, totals = weigh(scores, highest, head, begin)
        for g in range(GROUPS):
            part_mixed[head, g, span, :] = mixed[g]
            part_total[head, g, span, :] = totals[g]
            part_high[head, g, span, :] = jnp.broadcast_to(highest[g], (TILE, DH))

    def rest_extent(side, tile):
        begin = side * tile * TILE
        return begin, rows - begin

    def rest_scores(side, head, tile):
        return raw_scores(query_held[head, pl.ds(tile * TILE, TILE), :], head, *rest_extent(side, tile))

    def rest_finish(side, head, tile, raw):
        begin, count = rest_extent(side, tile)
        mask = bias[pl.ds(tile * TILE, TILE), pl.ds(begin, count)]
        rows_of = []
        if side == 0:
            for g in range(GROUPS):
                rows_of.append(stat_in[head, pl.ds(tile * GROUPS + g, 1), :])
        merge(head, tile, masked_scores(raw, mask), held[head, 1, pl.ds(begin, count), :], rows_of)

    def far_scores(tile):
        begin = tile * TILE
        keys = jnp.concatenate([far_held[0, pl.ds(begin, rows - begin), :], held[FORWARD, 0, received, :]], axis=0)
        return dot_keys(query_held[FORWARD, pl.ds(begin, TILE), :], keys)

    def far_finish(tile, raw):
        begin = tile * TILE
        mask = far_bias[pl.ds(begin, TILE), pl.ds(begin, 2 * rows - begin)]
        values = jnp.concatenate([far_held[1, pl.ds(begin, rows - begin), :], held[FORWARD, 1, received, :]], axis=0)
        merge(FORWARD, tile, masked_scores(raw, mask), values, [])

    def merge(head, tile, scores, values, level_rows):
        span = pl.ds(tile * TILE, TILE)
        tops, levels = [], []
        for g in range(GROUPS):
            top = jnp.maximum(part_high[head, g, span, :], jnp.max(scores[g], axis=-1, keepdims=True))
            if level_rows:
                level = jnp.sum(jnp.where(diagonal, level_rows[g], 0.0), axis=1, keepdims=True)
                top = jnp.maximum(top, level)
                levels.append(level)
            tops.append(top)
        wide = jnp.stack([jnp.concatenate([top] * (scores.shape[-1] // DH), axis=1) for top in tops])
        all_mixed, all_totals = mix(scores, wide, values)
        for g in range(GROUPS):
            scale = jnp.exp2(part_high[head, g, span, :] - tops[g])
            mixed = all_mixed[g] + part_mixed[head, g, span, :] * scale
            totals = all_totals[g] + part_total[head, g, span, :] * scale
            if level_rows:
                there = jnp.exp2(levels[g] - tops[g])
                mixed = mixed + held[head, g, span, :].astype(jnp.float32) * there
                totals = totals + there
            out_ref[span, pl.ds(pl.multiple_of(head * WIDTH, WIDTH) + g * DH, DH)] = (
                mixed * (1.0 / totals)
            ).astype(jnp.bfloat16)

    def pipelined(jobs):
        raw = jobs[0][0](*jobs[0][2])
        for at, (_, finish, job) in enumerate(jobs):
            later = None
            if at + 1 < len(jobs):
                later = jobs[at + 1][0](*jobs[at + 1][2])
            finish(*job, raw)
            raw = later

    def back(side, step, tile):
        return back_scores, back_finish, (step, side * SPLIT + step, tile)

    def part(side, head, tile):
        return part_scores, part_finish, (side, head, tile)

    def rest_jobs(side, step, at):
        return [(rest_scores, rest_finish, (side, at * SPLIT + step, tile)) for tile in range(tiles)]

    def rest(side, step, at):
        pipelined(rest_jobs(side, step, at))

    def rest_far():
        pipelined([(far_scores, far_finish, (tile,)) for tile in range(tiles)])

    def wait_direct(side, step):
        @pl.when(has_prev)
        def _():
            if step is SPLIT - 1:
                for tile in range(tiles):
                    span = pl.ds(tile * TILE, TILE)
                    slot_to_next(step, span, tile).wait_recv()
                    relay(step, side, span).start()
            else:
                slot_to_next(step, received).wait_recv()
                relay(step, side).start()
            if side == 0:
                stat_to_next(step, step).wait_recv()

    def wait_near():
        @pl.when(has_prev)
        def _():
            near_to_next().wait_recv()
            relay(SPLIT - 1, 1).start()

    def wait_far():
        @pl.when(has_prev)
        def _():
            far_to_next().wait_recv()
            relay(SPLIT - 1, 1).wait_recv()

    def wait_relayed(side, step):
        @pl.when(has_prev)
        def _():
            relay(step, 1 - side).wait_recv()
            if side == 0:
                stat_to_next(step, SPLIT + step).wait_recv()

    def wait_query(side, step, tile):
        @pl.when(has_next)
        def _():
            query_to_prev(step, 0, tile).wait_recv()

    def send_slot(side, step, tile):
        @pl.when(has_next)
        def _():
            slot_to_next(step, pl.ds(tile * TILE, TILE), tile).start()
            if tile == tiles - 1:
                stat_to_next(step, side * SPLIT + step).start()

    def run(side):
        last = SPLIT - 1
        first = 0
        if side == 1:
            from_core(0).wait_recv()
            from_core(SPLIT).wait_recv()
        pipelined([part(side, head, tile) for head in (0, SPLIT) for tile in range(tiles)])
        if side == 0:
            from_core(0).wait_recv()
            from_core(SPLIT).wait_recv()

        def backs(step, tile):
            return [back(side, step, tile)]

        @pl.loop(0, last)
        def _(step):
            from_core(step + 1).wait_recv()
            from_core(SPLIT + step + 1).wait_recv()
            for tile in range(first, tiles):
                wait_query(side, step, tile)
                jobs = backs(step, tile)
                for at in range(0 if tile == first else tile, tile + 1):
                    jobs.append(part(side, step + 1, at))
                    jobs.append(part(side, SPLIT + step + 1, at))
                pipelined(jobs)
                send_slot(side, step, tile)
                if tile == first:

                    @pl.when(step >= 2)
                    def _():
                        wait_direct(side, step - 2)
                        if side == 1:
                            wait_near()

            @pl.when(step >= 2)
            def _():
                rest(side, step - 2, side)
                wait_relayed(side, step - 2)
                rest(side, step - 2, 1 - side)

        if side == 0:
            for tile in range(tiles):
                wait_query(side, last, tile)
                jobs = backs(last, tile)
                if tile == 1:
                    jobs += rest_jobs(side, last - 2, 0)
                if tile == 3:
                    jobs += rest_jobs(side, last - 2, 1)
                pipelined(jobs)
                send_slot(side, last, tile)
                if tile == 0:
                    wait_direct(side, last - 2)
                if tile == 2:
                    wait_relayed(side, last - 2)
                    wait_direct(side, last - 1)

            wait_far()
            rest_far()
            rest(side, last - 1, 0)
            wait_relayed(side, last - 1)
            rest(side, last - 1, 1)
            wait_direct(side, last)
            rest(side, last, 0)
        else:
            wait_direct(side, last - 2)
            rest(side, last, 1)
            rest(side, last - 2, 1)
            wait_relayed(side, last - 2)
            wait_direct(side, last - 1)
            rest(side, last - 2, 0)
            rest(side, last - 1, 1)
            wait_relayed(side, last - 1)
            rest(side, last - 1, 0)
            wait_relayed(side, last)
            rest(side, last, 0)

    @pl.when(even)
    def _():
        run(0)

    @pl.when(odd)
    def _():
        run(1)

    @pl.loop(0, HK)
    def _(head):
        to_core(head).wait_send()

    @pl.when(has_next)
    def _():
        @pl.when(even)
        def _():
            far_to_next().wait_send()

        @pl.when(odd)
        def _():
            near_to_next().wait_send()

        for step in range(SPLIT):

            @pl.when(even)
            def _():
                slot_to_next(step, received).wait_send()
                stat_to_next(step, step).wait_send()

            @pl.when(jnp.logical_and(odd, step < SPLIT - 1))
            def _():
                slot_to_next(step, received).wait_send()
                stat_to_next(step, step).wait_send()

    @pl.when(has_prev)
    def _():
        for step in range(SPLIT):
            relay(step, core).wait_send()

        @pl.when(even)
        def _():
            for head in range(HK - 1):
                query_sent(head).wait_send()


def on_device(queries, keys, values, doc_lengths):
    rows = keys.shape[0]
    docs = doc_lengths.shape[0]
    shards = lax.axis_size("cp")
    stats = rows // TILE * GROUPS
    dma = pltpu.SemaphoreType.DMA
    hbm = pl.BlockSpec(memory_space=pltpu.HBM)
    return pl.pallas_call(
        functools.partial(kernel, shards),
        out_shape=pltpu.VMEM(queries.shape, queries.dtype),
        in_specs=[hbm] * 4,
        out_specs=pl.BlockSpec(memory_space=pltpu.VMEM),
        scratch_shapes=[
            pltpu.VMEM((HK, 2, 3 * rows, DH), keys.dtype),
            pltpu.VMEM((HK, rows, WIDTH), queries.dtype),
            pltpu.VMEM((SPLIT, rows, WIDTH), queries.dtype),
            pltpu.VMEM((2, rows, DH), keys.dtype),
            pltpu.VMEM((SPLIT, 2, rows, DH), keys.dtype),
            pltpu.VMEM((SPLIT, stats, TILE), jnp.float32),
            pltpu.VMEM((HK, stats, TILE), jnp.float32),
            pltpu.VMEM((rows, 3 * rows), jnp.float32),
            pltpu.VMEM((rows, 2 * rows), jnp.float32),
            pltpu.VMEM((rows, 2 * rows), jnp.float32),
            pltpu.VMEM((1, docs), jnp.int32),
            pltpu.VMEM((8, DH), jnp.float32),
            pltpu.VMEM((2 * rows, DH), keys.dtype),
            pltpu.VMEM((HK, GROUPS, rows, DH), jnp.float32),
            pltpu.VMEM((HK, GROUPS, rows, DH), jnp.float32),
            pltpu.VMEM((HK, GROUPS, rows, DH), jnp.float32),
            dma,
            dma,
            dma,
            dma((HK, 2)),
            dma((HK,)),
            dma((HK,)),
            dma((HK,)),
            dma((HK,)),
            dma((SPLIT, rows // TILE)),
            dma((SPLIT,)),
            dma((SPLIT + rows // TILE - 1,)),
            dma((SPLIT,)),
            dma((SPLIT,)),
            dma((SPLIT,)),
            dma((HK,)),
        ],
        compiler_params=pltpu.CompilerParams(
            collective_id=0, has_side_effects=True, vmem_limit_bytes=50 * 1024 * 1024
        ),
    )(*(pltpu.with_memory_space_constraint(x, pltpu.HBM) for x in (doc_lengths.reshape(1, docs), queries, keys, values)))


def solution(mesh):
    return jax.shard_map(
        on_device,
        mesh=mesh,
        in_specs=(P(("grp", "cp"), None), P(("grp", "cp"), None), P(("grp", "cp"), None), P("grp")),
        out_specs=P(("grp", "cp"), None),
        check_vma=False,
    )
```

```python
import functools
import math

import jax
import jax.numpy as jnp
from jax import lax
from jax.experimental import pallas as pl
from jax.experimental.pallas import tpu as pltpu
from jax.sharding import PartitionSpec as P

HQ = 16
HK = 8
DH = 128
GROUPS = HQ // HK
WIDTH = GROUPS * DH
TILE = 128
STACK = GROUPS * TILE
MASKED = -1e30
SPLIT = HK // 2
FORWARD = HK - 1
MESH = pl.DeviceIdType.MESH

LOG2E = math.log2(math.e)
exponent_scale = 144.0 ** (-0.5) * LOG2E


def kernel(
    shards,
    lengths_ref,
    queries_ref,
    keys_ref,
    values_ref,
    out_ref,
    held,
    query_held,
    query_back,
    far_held,
    slot,
    stat_out,
    stat_in,
    bias,
    back_bias,
    far_bias,
    lengths,
    mode,
    ones,
    part_mixed,
    part_total,
    part_high,
    lengths_sem,
    far_send,
    far_recv,
    load_sem,
    query_sem,
    core_send,
    core_recv,
    query_send,
    query_recv,
    slot_send,
    slot_recv,
    relay_send,
    relay_recv,
    stat_send,
    stat_recv,
):
    me = lax.axis_index("cp")
    core = lax.rem(me, 2)
    even = core == 0
    odd = core == 1
    partner = me + 1 - 2 * core
    rows = keys_ref.shape[0]
    docs = lengths_ref.shape[1]
    tiles = rows // TILE
    received = pl.ds(0, rows)
    own = pl.ds(pl.multiple_of((1 + core) * rows, rows), rows)
    has_prev = me >= 2
    has_next = me < shards - 2
    chip_begin = (me - core) * rows
    next_begin = chip_begin + 2 * rows

    def loads(head):
        lanes = pl.ds(pl.multiple_of(head * DH, DH), DH)
        return (
            pltpu.make_async_copy(keys_ref.at[:, lanes], held.at[head, 0, own], load_sem.at[head, 0]),
            pltpu.make_async_copy(values_ref.at[:, lanes], held.at[head, 1, own], load_sem.at[head, 1]),
        )

    def in_turn(turn):
        order = lax.rem(turn + HK - 1, HK)
        return lax.rem(order, 2) * SPLIT + order // 2

    def query_load(head):
        lanes = pl.ds(pl.multiple_of(head * WIDTH, WIDTH), WIDTH)
        return pltpu.make_async_copy(queries_ref.at[:, lanes], query_held.at[head], query_sem.at[head])

    def remote(source, target, send, recv, device):
        return pltpu.make_async_remote_copy(
            src_ref=source,
            dst_ref=target,
            send_sem=send,
            recv_sem=recv,
            device_id={"cp": device},
            device_id_type=MESH,
        )

    def to_core(head):
        return remote(held.at[head, :, own], held.at[head, :, own], core_send.at[head], core_recv.at[head], partner)

    def from_core(head):
        other = pl.ds(pl.multiple_of((2 - core) * rows, rows), rows)
        return remote(held.at[head, :, other], held.at[head, :, other], core_send.at[head], core_recv.at[head], partner)

    def query_to_prev(step, side, tile):
        span = pl.ds(tile * TILE, TILE)
        return remote(
            query_held.at[side * SPLIT + step, span],
            query_back.at[step, span],
            query_send.at[side * SPLIT + step],
            query_recv.at[step, tile],
            me - 2 + side,
        )

    def far_to_next():
        return remote(held.at[FORWARD, :, own], far_held, far_send, far_recv, me + 2)

    def near_to_next():
        return remote(
            held.at[FORWARD, :, own],
            held.at[FORWARD, :, received],
            slot_send.at[SPLIT - 1],
            slot_recv.at[SPLIT - 1],
            me + 2,
        )

    def query_sent(head):
        return remote(
            query_held.at[head], query_held.at[head], query_send.at[head], query_send.at[head], me - 2
        )

    def arrival(step, tile):
        return step + tile if step is SPLIT - 1 else step

    def slot_to_next(step, span, tile=0):
        return remote(
            slot.at[step, :, span],
            held.at[core * SPLIT + step, :, span],
            slot_send.at[step],
            slot_recv.at[arrival(step, tile)],
            me + 2,
        )

    def relay(step, side, span=received):
        head = side * SPLIT + step
        return remote(
            held.at[head, :, span], held.at[head, :, span], relay_send.at[step], relay_recv.at[step], partner
        )

    def stat_to_next(step, head):
        return remote(
            stat_out.at[step], stat_in.at[head], stat_send.at[step], stat_recv.at[head], me + 2 - core
        )

    barrier = pltpu.get_barrier_semaphore()

    def greet(device):
        pl.semaphore_signal(barrier, inc=1, device_id={"cp": device}, device_id_type=MESH)

    greet(partner)

    @pl.when(has_prev)
    def _():
        greet(me - core - 2)
        greet(me - core - 1)

    @pl.when(has_next)
    def _():
        greet(me - core + 2)
        greet(me - core + 3)

    @pl.loop(0, SPLIT)
    def _(step):
        query_load(step).start()
        query_load(SPLIT + step).start()

    lengths_load = pltpu.make_async_copy(lengths_ref, lengths, lengths_sem)
    lengths_load.start()

    @pl.loop(0, HK)
    def _(turn):
        for copy in loads(in_turn(turn)):
            copy.start()

    back_peers = jnp.where(has_prev, 2, 0)
    next_peers = jnp.where(has_next, 2, 0)
    pl.semaphore_wait(barrier, 1 + back_peers + next_peers)

    @pl.loop(0, SPLIT)
    def _(step):
        query_load(step).wait()
        query_load(SPLIT + step).wait()

        @pl.when(jnp.logical_and(even, has_prev))
        def _():
            for tile in range(tiles):
                query_to_prev(step, 0, tile).start()

                @pl.when(step < SPLIT - 1)
                def _():
                    query_to_prev(step, 1, tile).start()

    @pl.loop(0, HK)
    def _(turn):
        head = in_turn(turn)
        for copy in loads(head):
            copy.wait()

        @pl.when(jnp.logical_and(has_next, turn == 0))
        def _():
            @pl.when(even)
            def _():
                far_to_next().start()

            @pl.when(odd)
            def _():
                near_to_next().start()

        to_core(head).start()

    @pl.when(jnp.logical_not(has_prev))
    def _():
        held[:, :, received, :] = jnp.zeros((HK, 2, rows, DH), held.dtype)

        @pl.when(even)
        def _():
            far_held[...] = jnp.zeros(far_held.shape, far_held.dtype)
            stat_in[...] = jnp.full(stat_in.shape, MASKED, jnp.float32)

    ones[...] = jnp.ones(ones.shape, ones.dtype)
    stat_out[...] = jnp.full(stat_out.shape, MASKED, jnp.float32)

    lengths_load.wait()
    doc_row = lax.broadcasted_iota(jnp.int32, (docs, docs), 0)
    doc_lane = lax.broadcasted_iota(jnp.int32, (docs, docs), 1)
    length_row = lengths[...].astype(jnp.float32)
    length_column = jnp.sum(jnp.where(doc_row == doc_lane, length_row, 0.0), axis=1, keepdims=True)
    doc_ends = jnp.sum(jnp.where(doc_row <= doc_lane, length_column, 0.0), axis=0, keepdims=True)

    def doc_begins(positions):
        return jnp.max(jnp.where(positions >= doc_ends, doc_ends, 0.0), axis=1, keepdims=True)

    def boundary_begin(boundary):
        return doc_begins(jnp.full((8, 1), boundary, jnp.int32).astype(jnp.float32))

    def as_float(number):
        return jnp.full((1, 1), number, jnp.int32).astype(jnp.float32)

    row_iota = lax.broadcasted_iota(jnp.int32, (TILE, 1), 0)
    for tile in range(tiles):
        begins = doc_begins((next_begin + tile * TILE + row_iota).astype(jnp.float32))
        key_pos = (chip_begin + lax.broadcasted_iota(jnp.int32, (TILE, 2 * rows), 1)).astype(jnp.float32)
        back_bias[pl.ds(tile * TILE, TILE), :] = jnp.where(key_pos >= begins, 0.0, MASKED)

    next_wide = jnp.broadcast_to(boundary_begin(next_begin), (8, DH))
    mode[...] = next_wide

    begin_here = boundary_begin(chip_begin)[:1]
    here = as_float(chip_begin)
    floor = jnp.where(here - begin_here <= rows, 0.0, here)
    for tile in range(tiles):
        query_pos = (me * rows + tile * TILE + row_iota).astype(jnp.float32)
        begins = doc_begins(query_pos)
        far_pos = (chip_begin - 2 * rows + lax.broadcasted_iota(jnp.int32, (TILE, 2 * rows), 1)).astype(jnp.float32)
        far_bias[pl.ds(tile * TILE, TILE), :] = jnp.where(far_pos >= begins, 0.0, MASKED)
        begins = jnp.maximum(begins, floor)
        key_pos = (chip_begin - rows + lax.broadcasted_iota(jnp.int32, (TILE, 3 * rows), 1)).astype(jnp.float32)
        visible = (key_pos >= begins) & (key_pos <= query_pos)
        bias[pl.ds(tile * TILE, TILE), :] = jnp.where(visible, 0.0, MASKED)

    diagonal = lax.broadcasted_iota(jnp.int32, (TILE, TILE), 0) == lax.broadcasted_iota(
        jnp.int32, (TILE, TILE), 1
    )

    def stack(queries):
        return jnp.concatenate([queries[:, g * DH : (g + 1) * DH] for g in range(GROUPS)], axis=0)

    def dot_keys(queries, keys):
        return lax.dot_general(
            stack(queries), keys, (((1,), (1,)), ((), ())), preferred_element_type=jnp.float32
        )

    def raw_scores(queries, head, begin, count):
        return dot_keys(queries, held[head, 0, pl.ds(begin, count), :])

    def masked_scores(raw, mask):
        return raw.reshape(GROUPS, TILE, raw.shape[-1]) * exponent_scale + mask[None]

    def weigh(scores, highest, head, begin):
        return mix(scores, highest, held[head, 1, pl.ds(begin, scores.shape[-1]), :])

    def mix(scores, highest, values):
        count = scores.shape[-1]
        weights = jnp.exp2(scores - highest).astype(jnp.bfloat16).reshape(STACK, count)
        values = jnp.concatenate([values, ones[pl.ds(0, count), :]], axis=1)
        both = jnp.dot(weights, values, preferred_element_type=jnp.float32).reshape(GROUPS, TILE, 2 * DH)
        return both[:, :, :DH], both[:, :, DH:]

    def back_scores(step, head, tile):
        begin = rows + tile * TILE
        return raw_scores(query_back[step, pl.ds(tile * TILE, TILE), :], head, begin, 3 * rows - begin)

    def back_finish(step, head, tile, raw):
        begin = rows + tile * TILE
        span = pl.ds(tile * TILE, TILE)
        scores = masked_scores(raw, back_bias[span, pl.ds(tile * TILE, 2 * rows - tile * TILE)])
        highest = jnp.max(scores, axis=-1, keepdims=True)
        mixed, totals = weigh(scores, highest, head, begin)
        mixed = mixed * (1.0 / totals)
        level = highest + jnp.log2(totals)
        next_keys = as_float(next_begin) - mode[:1, :] <= rows
        for g in range(GROUPS):
            kept = held[head, g, pl.ds(2 * rows + tile * TILE, TILE), :].astype(jnp.float32)
            sent = jnp.where(next_keys, kept, mixed[g]).astype(jnp.bfloat16)
            row = jnp.sum(jnp.where(diagonal, level[g], 0.0), axis=0, keepdims=True)
            row = jnp.where(next_keys, MASKED, row)
            slot[step, g, span, :] = sent
            stat_out[step, pl.ds(tile * GROUPS + g, 1), :] = row

    def part_extent(side, tile):
        return rows, side * rows + (tile + 1) * TILE

    def part_scores(side, head, tile):
        return raw_scores(query_held[head, pl.ds(tile * TILE, TILE), :], head, *part_extent(side, tile))

    def part_finish(side, head, tile, raw):
        begin, count = part_extent(side, tile)
        span = pl.ds(tile * TILE, TILE)
        scores = masked_scores(raw, bias[span, pl.ds(begin, count)])
        highest = jnp.max(scores, axis=-1, keepdims=True)
        mixed, totals = weigh(scores, highest, head, begin)
        for g in range(GROUPS):
            part_mixed[head, g, span, :] = mixed[g]
            part_total[head, g, span, :] = totals[g]
            part_high[head, g, span, :] = jnp.broadcast_to(highest[g], (TILE, DH))

    def rest_extent(side, tile):
        begin = side * tile * TILE
        return begin, rows - begin

    def rest_scores(side, head, tile):
        return raw_scores(query_held[head, pl.ds(tile * TILE, TILE), :], head, *rest_extent(side, tile))

    def rest_finish(side, head, tile, raw):
        begin, count = rest_extent(side, tile)
        mask = bias[pl.ds(tile * TILE, TILE), pl.ds(begin, count)]
        rows_of = []
        if side == 0:
            for g in range(GROUPS):
                rows_of.append(stat_in[head, pl.ds(tile * GROUPS + g, 1), :])
        merge(head, tile, masked_scores(raw, mask), held[head, 1, pl.ds(begin, count), :], rows_of)

    def far_scores(tile):
        begin = tile * TILE
        keys = jnp.concatenate([far_held[0, pl.ds(begin, rows - begin), :], held[FORWARD, 0, received, :]], axis=0)
        return dot_keys(query_held[FORWARD, pl.ds(begin, TILE), :], keys)

    def far_finish(tile, raw):
        begin = tile * TILE
        mask = far_bias[pl.ds(begin, TILE), pl.ds(begin, 2 * rows - begin)]
        values = jnp.concatenate([far_held[1, pl.ds(begin, rows - begin), :], held[FORWARD, 1, received, :]], axis=0)
        merge(FORWARD, tile, masked_scores(raw, mask), values, [])

    def merge(head, tile, scores, values, level_rows):
        span = pl.ds(tile * TILE, TILE)
        tops, levels = [], []
        for g in range(GROUPS):
            top = jnp.maximum(part_high[head, g, span, :], jnp.max(scores[g], axis=-1, keepdims=True))
            if level_rows:
                level = jnp.sum(jnp.where(diagonal, level_rows[g], 0.0), axis=1, keepdims=True)
                top = jnp.maximum(top, level)
                levels.append(level)
            tops.append(top)
        wide = jnp.stack([jnp.concatenate([top] * (scores.shape[-1] // DH), axis=1) for top in tops])
        all_mixed, all_totals = mix(scores, wide, values)
        for g in range(GROUPS):
            scale = jnp.exp2(part_high[head, g, span, :] - tops[g])
            mixed = all_mixed[g] + part_mixed[head, g, span, :] * scale
            totals = all_totals[g] + part_total[head, g, span, :] * scale
            if level_rows:
                there = jnp.exp2(levels[g] - tops[g])
                mixed = mixed + held[head, g, span, :].astype(jnp.float32) * there
                totals = totals + there
            out_ref[span, pl.ds(pl.multiple_of(head * WIDTH, WIDTH) + g * DH, DH)] = (
                mixed * (1.0 / totals)
            ).astype(jnp.bfloat16)

    def pipelined(jobs):
        raw = jobs[0][0](*jobs[0][2])
        for at, (_, finish, job) in enumerate(jobs):
            later = None
            if at + 1 < len(jobs):
                later = jobs[at + 1][0](*jobs[at + 1][2])
            finish(*job, raw)
            raw = later

    def back(side, step, tile):
        return back_scores, back_finish, (step, side * SPLIT + step, tile)

    def part(side, head, tile):
        return part_scores, part_finish, (side, head, tile)

    def rest_jobs(side, step, at):
        return [(rest_scores, rest_finish, (side, at * SPLIT + step, tile)) for tile in range(tiles)]

    def rest(side, step, at):
        pipelined(rest_jobs(side, step, at))

    def far_jobs():
        return [(far_scores, far_finish, (tile,)) for tile in range(tiles)]

    def wait_direct(side, step):
        @pl.when(has_prev)
        def _():
            if step is SPLIT - 1:
                for tile in range(tiles):
                    span = pl.ds(tile * TILE, TILE)
                    slot_to_next(step, span, tile).wait_recv()
                    relay(step, side, span).start()
            else:
                slot_to_next(step, received).wait_recv()
                relay(step, side).start()
            if side == 0:
                stat_to_next(step, step).wait_recv()

    def wait_near():
        @pl.when(has_prev)
        def _():
            near_to_next().wait_recv()
            relay(SPLIT - 1, 1).start()

    def wait_far():
        @pl.when(has_prev)
        def _():
            far_to_next().wait_recv()
            relay(SPLIT - 1, 1).wait_recv()

    def wait_relayed(side, step):
        @pl.when(has_prev)
        def _():
            relay(step, 1 - side).wait_recv()
            if side == 0:
                stat_to_next(step, SPLIT + step).wait_recv()

    def wait_query(side, step, tile):
        @pl.when(has_next)
        def _():
            query_to_prev(step, 0, tile).wait_recv()

    def send_slot(side, step, tile):
        @pl.when(has_next)
        def _():
            slot_to_next(step, pl.ds(tile * TILE, TILE), tile).start()
            if tile == tiles - 1:
                stat_to_next(step, side * SPLIT + step).start()

    def run(side):
        last = SPLIT - 1
        first = 0
        if side == 1:
            from_core(0).wait_recv()
            from_core(SPLIT).wait_recv()
        pipelined([part(side, head, tile) for head in (0, SPLIT) for tile in range(tiles)])
        if side == 0:
            from_core(0).wait_recv()
            from_core(SPLIT).wait_recv()

        def backs(step, tile):
            return [back(side, step, tile)]

        @pl.loop(0, last)
        def _(step):
            from_core(step + 1).wait_recv()
            from_core(SPLIT + step + 1).wait_recv()
            for tile in range(first, tiles):
                wait_query(side, step, tile)
                jobs = backs(step, tile)
                for at in range(0 if tile == first else tile, tile + 1):
                    jobs.append(part(side, step + 1, at))
                    jobs.append(part(side, SPLIT + step + 1, at))
                pipelined(jobs)
                send_slot(side, step, tile)
                if tile == first:

                    @pl.when(step >= 2)
                    def _():
                        wait_direct(side, step - 2)
                        if side == 1:
                            wait_near()

            @pl.when(step >= 2)
            def _():
                rest(side, step - 2, side)
                wait_relayed(side, step - 2)
                rest(side, step - 2, 1 - side)

        if side == 0:
            for tile in range(tiles):
                wait_query(side, last, tile)
                jobs = backs(last, tile)
                if tile == 1:
                    jobs += rest_jobs(side, last - 2, 0)
                if tile == 3:
                    jobs += rest_jobs(side, last - 2, 1)
                pipelined(jobs)
                send_slot(side, last, tile)
                if tile == 0:
                    wait_direct(side, last - 2)
                if tile == 2:
                    wait_relayed(side, last - 2)
                    wait_direct(side, last - 1)

            wait_relayed(side, last - 1)
            pipelined(rest_jobs(side, last - 1, 0) + rest_jobs(side, last - 1, 1))
            wait_direct(side, last)
            wait_far()
            pipelined(far_jobs() + rest_jobs(side, last, 0))
        else:
            wait_direct(side, last - 2)
            pipelined(rest_jobs(side, last, 1) + rest_jobs(side, last - 2, 1))
            wait_relayed(side, last - 2)
            wait_direct(side, last - 1)
            pipelined(rest_jobs(side, last - 2, 0) + rest_jobs(side, last - 1, 1))
            wait_relayed(side, last - 1)
            rest(side, last - 1, 0)
            wait_relayed(side, last)
            rest(side, last, 0)

    @pl.when(even)
    def _():
        run(0)

    @pl.when(odd)
    def _():
        run(1)

    @pl.loop(0, HK)
    def _(head):
        to_core(head).wait_send()

    @pl.when(has_next)
    def _():
        @pl.when(even)
        def _():
            far_to_next().wait_send()

        @pl.when(odd)
        def _():
            near_to_next().wait_send()

        for step in range(SPLIT):

            @pl.when(even)
            def _():
                slot_to_next(step, received).wait_send()
                stat_to_next(step, step).wait_send()

            @pl.when(jnp.logical_and(odd, step < SPLIT - 1))
            def _():
                slot_to_next(step, received).wait_send()
                stat_to_next(step, step).wait_send()

    @pl.when(has_prev)
    def _():
        for step in range(SPLIT):
            relay(step, core).wait_send()

        @pl.when(even)
        def _():
            for head in range(HK - 1):
                query_sent(head).wait_send()


def on_device(queries, keys, values, doc_lengths):
    rows = keys.shape[0]
    docs = doc_lengths.shape[0]
    shards = lax.axis_size("cp")
    stats = rows // TILE * GROUPS
    dma = pltpu.SemaphoreType.DMA
    hbm = pl.BlockSpec(memory_space=pltpu.HBM)
    return pl.pallas_call(
        functools.partial(kernel, shards),
        out_shape=pltpu.VMEM(queries.shape, queries.dtype),
        in_specs=[hbm] * 4,
        out_specs=pl.BlockSpec(memory_space=pltpu.VMEM),
        scratch_shapes=[
            pltpu.VMEM((HK, 2, 3 * rows, DH), keys.dtype),
            pltpu.VMEM((HK, rows, WIDTH), queries.dtype),
            pltpu.VMEM((SPLIT, rows, WIDTH), queries.dtype),
            pltpu.VMEM((2, rows, DH), keys.dtype),
            pltpu.VMEM((SPLIT, 2, rows, DH), keys.dtype),
            pltpu.VMEM((SPLIT, stats, TILE), jnp.float32),
            pltpu.VMEM((HK, stats, TILE), jnp.float32),
            pltpu.VMEM((rows, 3 * rows), jnp.float32),
            pltpu.VMEM((rows, 2 * rows), jnp.float32),
            pltpu.VMEM((rows, 2 * rows), jnp.float32),
            pltpu.VMEM((1, docs), jnp.int32),
            pltpu.VMEM((8, DH), jnp.float32),
            pltpu.VMEM((2 * rows, DH), keys.dtype),
            pltpu.VMEM((HK, GROUPS, rows, DH), jnp.float32),
            pltpu.VMEM((HK, GROUPS, rows, DH), jnp.float32),
            pltpu.VMEM((HK, GROUPS, rows, DH), jnp.float32),
            dma,
            dma,
            dma,
            dma((HK, 2)),
            dma((HK,)),
            dma((HK,)),
            dma((HK,)),
            dma((HK,)),
            dma((SPLIT, rows // TILE)),
            dma((SPLIT,)),
            dma((SPLIT + rows // TILE - 1,)),
            dma((SPLIT,)),
            dma((SPLIT,)),
            dma((SPLIT,)),
            dma((HK,)),
        ],
        compiler_params=pltpu.CompilerParams(
            collective_id=0, has_side_effects=True, vmem_limit_bytes=50 * 1024 * 1024
        ),
    )(*(pltpu.with_memory_space_constraint(x, pltpu.HBM) for x in (doc_lengths.reshape(1, docs), queries, keys, values)))


def solution(mesh):
    return jax.shard_map(
        on_device,
        mesh=mesh,
        in_specs=(P(("grp", "cp"), None), P(("grp", "cp"), None), P(("grp", "cp"), None), P("grp")),
        out_specs=P(("grp", "cp"), None),
        check_vma=False,
    )
```
